32 devices in a mesh: dp: 8 (over z, y), mp: 4 (over x, core).
Axes of the slice: x: 2, y: 2, z: 4, core: 2. Of those that a mesh axis runs over, the one named last changes fastest.
Arguments:
- patch_query: bfloat16 [2048, 4096], P('dp'), may hold values from -6 to 6
- key_cache: bfloat16 [2048, 16, 4096], P('dp', None, 'mp'), may hold values from -48 to 48
- value_cache: bfloat16 [2048, 16, 4096], P('dp', None, 'mp'), may hold values from -6 to 6
- cache_len: int32 [2048], P('dp'), may hold values from 1 to 16
- patch_end: int32 [2048], P('dp'), may hold values from 0 to 1, as said below
- ended_index: int32 [1024], P('dp'), may hold values from 0 to 256, as said below
- pool_out: bfloat16 [4096, 4096], P('mp'), may hold values from -0.09375 to 0.09375
- norm_gain: float32 [2, 4096], replicated, may hold values from 0.1 to 1.9
- w_in: bfloat16 [2, 4096, 2, 14336], P(None, 'dp', None, 'mp'), may hold values from -0.09375 to 0.09375
- w_out: bfloat16 [2, 14336, 4096], P(None, 'mp', 'dp'), may hold values from -0.046875 to 0.046875
Outputs:
- global_out: bfloat16 [2048, 4096], P('dp')
The draws below stay inside these ranges and needn't reach their ends.
Inputs may be any that keep to these rules, and one draw needn't show every extreme that they name: `patch_end`: each index of dp has at most 128 ended patches among its 256 sequences, and some index has exactly 128. `ended_index`: each aligned block of 128 entries lists, in increasing order, the local indices of the ended sequences of that index of dp, then 256 in the remaining entries.
All inputs are finite; a program needn't handle non-finite values.
Results may differ from the reference program's by a relative error of at most 0.024.
Values may be sent and summed in bfloat16 or wider, within the bound.
A program may use at most 128 MiB of HBM per device.

```python
import jax
import jax.numpy as jnp
from jax import lax

D = 4096
FF = 14336
HEAD_DIM = 128
LAYERS = 2
PATCH = 16
SEQ_DEV = 256
CAP = 128
B = 2048
R = 1024
N_DP = 8
N_MP = 4


def query_and_keys(key):
    query_draw = jnp.clip(jax.random.normal(jax.random.fold_in(key, 11), (B, D), jnp.float32), -6.0, 6.0)
    keys_draw = jnp.clip(jax.random.normal(jax.random.fold_in(key, 12), (B, PATCH, D), jnp.float32), -6.0, 6.0)
    return (query_draw, keys_draw)


def draw_patch_query(key, part):
    return query_and_keys(key)[0].astype(jnp.bfloat16)


def draw_key_cache(key, part):
    return query_and_keys(key)[1].astype(jnp.bfloat16)


def ended_tables(key):
    shards = B // SEQ_DEV
    shard_keys = jax.random.split(jax.random.fold_in(key, 21), shards)
    counts = jax.random.randint(jax.random.fold_in(key, 22), (shards,), CAP // 4, CAP + 1)
    fullest = jax.random.randint(jax.random.fold_in(key, 23), (), 0, shards)
    counts = counts.at[fullest].set(CAP)

    def single_shard(shard_key, ended_count):
        permuted = jax.random.permutation(shard_key, SEQ_DEV)
        ranking = jnp.argsort(permuted, stable=True)
        flagged = (ranking < ended_count).astype(jnp.int32)
        position = jnp.cumsum(flagged) - 1
        target = jnp.where(flagged == 1, position, CAP)
        slot_index = jnp.full((CAP,), SEQ_DEV, jnp.int32).at[target].set(jnp.arange(SEQ_DEV, dtype=jnp.int32), mode='drop')
        return (flagged, slot_index)
    flagged, slot_index = jax.vmap(single_shard)(shard_keys, counts)
    return (flagged.reshape(-1).astype(jnp.int32), slot_index.reshape(-1).astype(jnp.int32))


def draw_patch_end(key, part):
    return ended_tables(key)[0]


def draw_ended_index(key, part):
    return ended_tables(key)[1]


def plant(drawn, rng, smallest, largest):
    index_at = [jax.random.randint(jax.random.fold_in(rng, axis), (), 0, length) for axis, length in enumerate(drawn.shape)]
    longest = drawn.shape.index(max(drawn.shape))
    beside = index_at[:longest] + [(index_at[longest] + 1) % drawn.shape[longest]] + index_at[longest + 1:]
    return drawn.at[tuple(index_at)].set(smallest).at[tuple(beside)].set(largest)


def levels(stream_key, dims, pieces, low, largest):
    factor_of, own = 1.0, jax.random.fold_in(stream_key, 6)
    for dim, parts in pieces:
        draws = jnp.exp(jax.random.uniform(jax.random.fold_in(own, dim), (parts,), jnp.float32, low / len(pieces), largest / len(pieces)))
        factor_of = factor_of * jnp.repeat(draws, dims[dim] // parts).reshape([-1 if axis == dim else 1 for axis in range(len(dims))])
    return factor_of


def gaussian(rng, dims, scale, most, pieces=(), held_as=jnp.bfloat16):
    values = scale * jax.random.normal(rng, dims, jnp.float32)
    if pieces:
        values = values * levels(rng, dims, pieces, -0.22, 0.18)
    return jnp.clip(values, -most, most).astype(held_as)


def setup_inputs(seed: int = 0) -> dict:
    streams_of = jax.random.split(jax.random.key(seed), 11)
    return {
        "patch_query": draw_patch_query(jax.random.fold_in(streams_of[10], 71), 0),
        "key_cache": draw_key_cache(jax.random.fold_in(streams_of[10], 71), 0),
        "value_cache": gaussian(streams_of[2], (B, PATCH, D), 1.0, 6.0, ((0, 8), (2, 4))),
        "cache_len": plant(jax.random.randint(streams_of[3], (B,), 1, PATCH + 1), jax.random.fold_in(streams_of[3], 1), 1, PATCH).astype(jnp.int32),
        "patch_end": draw_patch_end(jax.random.fold_in(streams_of[10], 71), 0),
        "ended_index": draw_ended_index(jax.random.fold_in(streams_of[10], 71), 0),
        "pool_out": gaussian(streams_of[6], (D, D), D ** -0.5, 0.09375, ((0, 4),)),
        "norm_gain": jnp.clip(1.0 + 0.18 * jax.random.normal(streams_of[7], (LAYERS, D), jnp.float32), 0.1, 1.9),
        "w_in": gaussian(streams_of[8], (LAYERS, D, 2, FF), D ** -0.5, 0.09375, ((1, 8), (3, 4))),
        "w_out": gaussian(streams_of[9], (LAYERS, FF, D), FF ** -0.5, 0.046875, ((1, 4), (2, 8))),
    }


norm_floor = 1e-05

def rounded(value):
    return lax.optimization_barrier(value.astype(jnp.bfloat16)).astype(jnp.float32)

def attend_all(query, keys, values, lengths):
    total_rows, patch_len, full_width = keys.shape
    head_count = full_width // HEAD_DIM
    query_heads = query.astype(jnp.float32).reshape(total_rows, head_count, HEAD_DIM)
    key_heads = keys.astype(jnp.float32).reshape(total_rows, patch_len, head_count, HEAD_DIM)
    value_heads = values.astype(jnp.float32).reshape(total_rows, patch_len, head_count, HEAD_DIM)
    scores = jnp.einsum('shd,sphd->shp', query_heads, key_heads, precision=lax.Precision.HIGHEST) * HEAD_DIM ** (-0.5)
    live_mask = jnp.arange(patch_len, dtype=jnp.int32)[None, None, :] < lengths[:, None, None]
    scores = jnp.where(live_mask, scores, jnp.float32(-1e+30))
    top_score = lax.optimization_barrier(jnp.max(scores, axis=2, keepdims=True))
    expo = jnp.where(live_mask, jnp.exp(scores - top_score), jnp.float32(0.0))
    weights = (expo / lax.optimization_barrier(jnp.sum(expo, axis=2, keepdims=True))).astype(jnp.bfloat16)
    mixed = jnp.einsum('shp,sphd->shd', weights.astype(jnp.float32), value_heads, precision=lax.Precision.HIGHEST)
    return mixed.astype(jnp.bfloat16).reshape(total_rows, full_width)

def blocked_product(left, right, blocks):
    rows = left.shape[0]
    inner = left.shape[1] // blocks
    left_blocks = left.reshape(rows, blocks, inner)
    right_blocks = right.reshape(blocks, inner, right.shape[1])

    def add_block(index, carry):
        left_part = lax.dynamic_index_in_dim(left_blocks, index, 1, keepdims=False).astype(jnp.float32)
        right_part = lax.dynamic_index_in_dim(right_blocks, index, 0, keepdims=False).astype(jnp.float32)
        term = jnp.dot(left_part, right_part, precision=lax.Precision.HIGHEST, preferred_element_type=jnp.float32)
        return carry + rounded(term)
    start_value = jnp.zeros((rows, right.shape[1]), jnp.float32)
    return lax.fori_loop(0, blocks, add_block, start_value)

def reference(patch_query, key_cache, value_cache, cache_len, patch_end, ended_index, pool_out, norm_gain, w_in, w_out):
    attended = attend_all(patch_query, key_cache, value_cache, cache_len)
    pooled = patch_query.astype(jnp.float32) + blocked_product(attended, pool_out, N_MP)
    owner = jnp.arange(R, dtype=jnp.int32) // CAP
    valid = ended_index < SEQ_DEV
    rows = (owner * SEQ_DEV + jnp.minimum(ended_index, SEQ_DEV - 1)).astype(jnp.int32)
    state = jnp.where(valid[:, None], pooled[rows], jnp.float32(0.0))
    for layer_idx in range(LAYERS):
        mean_square = lax.optimization_barrier(jnp.mean(state * state, axis=1, keepdims=True))
        normed = (state * lax.rsqrt(mean_square + norm_floor) * norm_gain[layer_idx][None, :]).astype(jnp.bfloat16)
        gate_up = blocked_product(normed, w_in[layer_idx].reshape(D, 2 * FF), N_DP)
        hidden = (jax.nn.silu(gate_up[:, :FF]) * gate_up[:, FF:]).astype(jnp.bfloat16)
        ffn = blocked_product(hidden, w_out[layer_idx], N_MP).astype(jnp.bfloat16)
        state = state + ffn.astype(jnp.float32)
    placed = jnp.zeros((B, D), jnp.float32).at[rows].add(jnp.where(valid[:, None], state, jnp.float32(0.0)))
    return (placed * patch_end.astype(jnp.float32)[:, None]).astype(jnp.bfloat16)
```

```python
import functools

import jax
import jax.numpy as jnp
from jax import lax
from jax.experimental import pallas as pl
from jax.experimental.pallas import tpu as pltpu
from jax.sharding import PartitionSpec as P

HEAD_DIM = 128
LANES = 128
LEAD = 4


norm_floor = 1e-05


def attend_local(query_cols, keys, values, lengths):
    seq_rows, patch_len, heads_width = keys.shape
    head_count = heads_width // HEAD_DIM
    query_heads = query_cols.reshape(seq_rows, head_count, HEAD_DIM)
    key_heads = keys.reshape(seq_rows, patch_len, head_count, HEAD_DIM)
    value_heads = values.reshape(seq_rows, patch_len, head_count, HEAD_DIM)
    scores = jnp.einsum(
        "shd,sphd->shp", query_heads, key_heads, preferred_element_type=jnp.float32
    ) * HEAD_DIM ** (-0.5)
    live_mask = jnp.arange(patch_len, dtype=jnp.int32)[None, None, :] < lengths[:, None, None]
    scores = jnp.where(live_mask, scores, jnp.float32(-1e30))
    top_score = jnp.max(scores, axis=2, keepdims=True)
    expo = jnp.where(live_mask, jnp.exp(scores - top_score), jnp.float32(0.0))
    weights = (expo / jnp.sum(expo, axis=2, keepdims=True)).astype(jnp.bfloat16)
    mixed = jnp.einsum("shp,sphd->shd", weights, value_heads, preferred_element_type=jnp.float32)
    return mixed.astype(jnp.bfloat16).reshape(seq_rows, heads_width)


def swap(value, axis, size, bit):
    return lax.ppermute(value, axis, [(i, i ^ bit) for i in range(size)])


def own_rows_of_sum(value, size):
    place = lax.axis_index("mp")
    bit = 1
    total = value.astype(jnp.float32)
    while bit < size:
        half = total.shape[0] // 2
        low = (place // bit) % 2
        kept = lax.dynamic_slice_in_dim(total, low * half, half, 0)
        given = lax.dynamic_slice_in_dim(total, (1 - low) * half, half, 0).astype(jnp.bfloat16)
        total = kept + swap(given, "mp", size, bit).astype(jnp.float32)
        bit *= 2
    return total


def layers_kernel(
    n_dp, n_mp, state_in, gain_ref, win_ref, wout_ref, out_ref,
    state, normed, feats, acc, w_up, w_down, right_buf, left_buf, right_hid, left_hid,
    give, got, share, back, final,
    wl_sem, ws_sem, wr_sem, ol_sem, os_sem, or_sem,
    rs_sem, rr_sem, ls_sem, lr_sem, hrs_sem, hrr_sem, hls_sem, hlr_sem,
    az_s, az_r, ag_s, ag_r, dd_s, dd_r, dz_s, dz_r, ff_s, ff_r,
):
    layers, chunks, full_width, pair_cols = w_up.shape
    line = n_dp // 2
    bits = n_mp.bit_length() - 1
    block_cols = full_width // 2
    own = state.shape[0]
    stripe = line * own
    half_rows = right_buf.shape[1]
    dp, mp = lax.axis_index("dp"), lax.axis_index("mp")
    z, y = dp // 2, dp % 2
    top = line - 1
    reverse = 0
    for i in range(bits):
        reverse = reverse + ((mp // (1 << i)) % 2) * (1 << (bits - 1 - i))
    block = reverse * 2 + y

    def flip(value, bit):
        return value + bit - 2 * bit * ((value // bit) % 2)

    def partner(t):
        if t == 0:
            return (dp + 1 - 2 * y, mp)
        return (dp, flip(mp, 1 << (bits - t)))

    def at_line(other):
        return (other * 2 + y, mp)

    def send(src, dst, s_sem, r_sem, device):
        return pltpu.make_async_remote_copy(
            src_ref=src, dst_ref=dst, send_sem=s_sem, recv_sem=r_sem,
            device_id=device, device_id_type=pl.DeviceIdType.MESH,
        )

    barrier = pltpu.get_barrier_semaphore()
    for d in range(1, line):
        pl.semaphore_signal(
            barrier, inc=1, device_id=at_line((z + d) % line), device_id_type=pl.DeviceIdType.MESH
        )
    for t in range(bits + 1):
        pl.semaphore_signal(barrier, inc=1, device_id=partner(t), device_id_type=pl.DeviceIdType.MESH)
    pl.semaphore_wait(barrier, line - 1 + bits + 1)

    def own_up(l, q):
        return pltpu.make_async_copy(
            win_ref.at[l, y * chunks + q],
            w_up.at[l, q, pl.ds(y * block_cols, block_cols), :],
            wl_sem.at[l * chunks + q],
        )

    def own_down(l, q):
        return pltpu.make_async_copy(
            wout_ref.at[l, pl.ds((y * chunks + q) * LANES, LANES), :],
            w_down.at[l, q, y],
            ol_sem.at[l * chunks + q],
        )

    def give_up(l, q):
        return send(
            win_ref.at[l, (1 - y) * chunks + q],
            w_up.at[l, q, pl.ds(y * block_cols, block_cols), :],
            ws_sem.at[l * chunks + q], wr_sem.at[l * chunks + q], partner(0),
        )

    def give_down(l, q):
        return send(
            wout_ref.at[l, pl.ds(((1 - y) * chunks + q) * LANES, LANES), :],
            w_down.at[l, q, y],
            os_sem.at[l * chunks + q], or_sem.at[l * chunks + q], partner(0),
        )

    def issue(piece):
        l, q = piece // chunks, piece % chunks
        give_up(l, q).start()
        give_down(l, q).start()

    def start_own(piece, carry):
        own_up(piece // chunks, piece % chunks).start()
        own_down(piece // chunks, piece % chunks).start()
        return carry

    pieces = layers * chunks
    lead = min(LEAD, pieces)

    def start_lead(piece, carry):
        issue(piece)
        return carry

    lax.fori_loop(0, lead, start_lead, 0)
    lax.fori_loop(0, pieces, start_own, 0)

    state[...] = state_in[...]
    first_use = jnp.minimum(z, top - z)
    first_down = jnp.minimum(z, top - z) + top + 1
    steps = chunks + 2 * top + 2
    early = chunks + 2

    def one_layer(l, carry):
        value = state[...]
        scale = lax.rsqrt(jnp.mean(value * value, axis=1, keepdims=True) + norm_floor)
        normed[...] = (value * scale * gain_ref[pl.ds(l, 1), :]).astype(jnp.bfloat16)
        mine = block * stripe + z * own
        for d in range(1, line):
            other = (z + d) % line
            send(
                normed.at[:, pl.ds(pl.multiple_of(other * full_width, LANES), full_width)],
                feats.at[pl.ds(pl.multiple_of(mine, own), own), :],
                az_s.at[d], az_r.at[d], at_line(other),
            ).start()
        feats[pl.ds(pl.multiple_of(mine, own), own), :] = normed[
            :, pl.ds(pl.multiple_of(z * full_width, LANES), full_width)
        ]
        for d in range(1, line):
            send(
                normed.at[:, pl.ds(0, full_width)], feats.at[pl.ds(0, own), :],
                az_s.at[d], az_r.at[d], at_line((z + d) % line),
            ).wait()
        for t in range(bits + 1):
            rows = stripe << t
            start = pl.multiple_of((block // (1 << t)) * rows, stripe)
            ref = feats.at[pl.ds(start, rows), :]
            step = send(ref, ref, ag_s.at[t], ag_r.at[t], partner(t))
            step.start()
            step.wait()

        acc[...] = jnp.zeros_like(acc)

        def hidden_of(total):
            gate, up = total[:, :LANES], total[:, LANES:]
            return (gate / (1.0 + jnp.exp(-gate)) * up).astype(jnp.bfloat16)

        def chain(q, row0, first, last, to_next, to_prev, buf, hid, s_s, s_r, h_s, h_r):
            part = jnp.dot(
                feats[row0 : row0 + half_rows, :], w_up[l, q], preferred_element_type=jnp.float32
            )

            @pl.when(z == first)
            def _():
                buf[q] = part.astype(jnp.bfloat16)

            @pl.when(z != first)
            def _():
                send(buf.at[q], buf.at[q], s_s.at[q], s_r.at[q], at_line(to_next)).wait_recv()

            @pl.when(jnp.logical_and(z != first, z != last))
            def _():
                buf[q] = (part + buf[q].astype(jnp.float32)).astype(jnp.bfloat16)

            @pl.when(z == last)
            def _():
                hid[q] = hidden_of(part + buf[q].astype(jnp.float32))
                send(hid.at[q], hid.at[q], h_s.at[q], h_r.at[q], at_line(to_prev)).start()

            @pl.when(z != last)
            def _():
                send(buf.at[q], buf.at[q], s_s.at[q], s_r.at[q], at_line(to_next)).start()

        def pass_on(q, first, last, to_prev, hid, h_s, h_r):
            @pl.when(z != last)
            def _():
                send(hid.at[q], hid.at[q], h_s.at[q], h_r.at[q], at_line(to_prev)).wait_recv()

            @pl.when(jnp.logical_and(z != last, z != first))
            def _():
                send(hid.at[q], hid.at[q], h_s.at[q], h_r.at[q], at_line(to_prev)).start()

        def down(q, row0, hid):
            for c in range(2):
                cols = slice(c * block_cols, (c + 1) * block_cols)
                acc[row0 : row0 + half_rows, cols] += jnp.dot(
                    hid[q], w_down[l, q, c], preferred_element_type=jnp.float32
                )

        nxt, prv = jnp.minimum(z + 1, top), jnp.maximum(z - 1, 0)

        def within(q):
            return jnp.logical_and(q >= 0, q < chunks)

        def one_step(s, inner):
            qw = s - first_use

            @pl.when(within(qw))
            def _():
                own_up(l, qw).wait()
                give_up(l, qw).wait_recv()

            qd = s - first_down

            @pl.when(within(qd))
            def _():
                own_down(l, qd).wait()
                give_down(l, qd).wait_recv()

            qr = s - z

            @pl.when(within(qr))
            def _():
                chain(qr, 0, 0, top, nxt, prv, right_buf, right_hid,
                      rs_sem, rr_sem, hrs_sem, hrr_sem)

            ql = s - (top - z)

            @pl.when(within(ql))
            def _():
                chain(ql, half_rows, top, 0, prv, nxt, left_buf, left_hid,
                      ls_sem, lr_sem, hls_sem, hlr_sem)

            hr = s - (top + 1) - (top - z)

            @pl.when(within(hr))
            def _():
                pass_on(hr, 0, top, prv, right_hid, hrs_sem, hrr_sem)

            hl = s - (top + 1) - z

            @pl.when(within(hl))
            def _():
                pass_on(hl, top, 0, nxt, left_hid, hls_sem, hlr_sem)

            piece = lead + s + l * early

            @pl.when(jnp.logical_and(jnp.logical_or(l > 0, s < early), piece < pieces))
            def _():
                issue(piece)

            @pl.when(within(hr))
            def _():
                down(hr, 0, right_hid)

            @pl.when(within(hl))
            def _():
                down(hl, half_rows, left_hid)

            return inner

        lax.fori_loop(0, steps, one_step, 0)

        def drain(q, inner):
            @pl.when(z != top)
            def _():
                send(right_buf.at[q], right_buf.at[q], rs_sem.at[q], rr_sem.at[q],
                     at_line(nxt)).wait_send()

            @pl.when(z != 0)
            def _():
                send(left_buf.at[q], left_buf.at[q], ls_sem.at[q], lr_sem.at[q],
                     at_line(prv)).wait_send()

            @pl.when(z != 0)
            def _():
                send(right_hid.at[q], right_hid.at[q], hrs_sem.at[q], hrr_sem.at[q],
                     at_line(prv)).wait_send()

            @pl.when(z != top)
            def _():
                send(left_hid.at[q], left_hid.at[q], hls_sem.at[q], hlr_sem.at[q],
                     at_line(nxt)).wait_send()

            return inner

        lax.fori_loop(0, chunks, drain, 0)

        for t in range(bits, -1, -1):
            rows = stripe << t
            at = stripe * ((1 << t) - 1)
            side = (block // (1 << t)) % 2
            here = pl.multiple_of((block // (1 << t)) * rows, stripe)
            there = pl.multiple_of((block // (1 << t) + 1 - 2 * side) * rows, stripe)
            give[at : at + rows, :] = acc[pl.ds(there, rows), :].astype(jnp.bfloat16)
            step = send(
                give.at[pl.ds(at, rows), :], got.at[pl.ds(at, rows), :],
                dd_s.at[t], dd_r.at[t], partner(t),
            )
            step.start()
            step.wait()
            acc[pl.ds(here, rows), :] += got[at : at + rows, :].astype(jnp.float32)
        share[...] = acc[pl.ds(pl.multiple_of(block * stripe, stripe), stripe), :].astype(jnp.bfloat16)
        columns = pl.ds(pl.multiple_of(z * full_width, LANES), full_width)
        for d in range(1, line):
            other = (z + d) % line
            send(
                share.at[pl.ds(pl.multiple_of(other * own, own), own), :], back.at[:, columns],
                dz_s.at[d], dz_r.at[d], at_line(other),
            ).start()
        back[:, columns] = share[pl.ds(pl.multiple_of(z * own, own), own), :]
        for d in range(1, line):
            send(
                share.at[pl.ds(0, own), :], back.at[:, pl.ds(0, full_width)],
                dz_s.at[d], dz_r.at[d], at_line((z + d) % line),
            ).wait()
        state[...] += back[...].astype(jnp.float32)
        return carry

    lax.fori_loop(0, layers, one_layer, 0)

    def drain_weights(piece, carry):
        give_up(piece // chunks, piece % chunks).wait_send()
        give_down(piece // chunks, piece % chunks).wait_send()
        return carry

    lax.fori_loop(0, pieces, drain_weights, 0)

    final[pl.ds(pl.multiple_of(reverse * own, own), own), :] = state[...].astype(jnp.bfloat16)
    for t in range(bits):
        rows = own << t
        ref = final.at[pl.ds(pl.multiple_of((reverse // (1 << t)) * rows, own), rows), :]
        step = send(ref, ref, ff_s.at[t], ff_r.at[t], partner(t + 1))
        step.start()
        step.wait()
    out_ref[...] = final[...]


def run_layers(n_dp, n_mp, state, norm_gain, win, wout):
    layers, twice, block_cols, pair_cols = win.shape
    own, features = state.shape
    chunks = twice // 2
    line = n_dp // 2
    bits = n_mp.bit_length() - 1
    width = 2 * block_cols
    rows = own * line * 2 * n_mp
    half = rows // 2
    slots = own * n_mp
    dma = pltpu.SemaphoreType.DMA
    vmem = pltpu.VMEM
    bf16, f32 = jnp.bfloat16, jnp.float32
    stripe = own * line
    passing = stripe * (2 * n_mp - 1)
    flops = 2 * layers * rows * chunks * LANES * 3 * width
    return pl.pallas_call(
        functools.partial(layers_kernel, n_dp, n_mp),
        name="global_layers",
        out_shape=jax.ShapeDtypeStruct((slots, features), bf16),
        in_specs=[
            pl.BlockSpec(memory_space=pltpu.VMEM),
            pl.BlockSpec(memory_space=pltpu.VMEM),
            pl.BlockSpec(memory_space=pl.ANY),
            pl.BlockSpec(memory_space=pl.ANY),
        ],
        out_specs=pl.BlockSpec(memory_space=pltpu.VMEM),
        scratch_shapes=[
            vmem((own, features), f32),
            vmem((own, features), bf16),
            vmem((rows, width), bf16),
            vmem((rows, width), f32),
            vmem((layers, chunks, width, pair_cols), bf16),
            vmem((layers, chunks, 2, LANES, block_cols), bf16),
            vmem((chunks, half, pair_cols), bf16),
            vmem((chunks, half, pair_cols), bf16),
            vmem((chunks, half, LANES), bf16),
            vmem((chunks, half, LANES), bf16),
            vmem((passing, width), bf16),
            vmem((passing, width), bf16),
            vmem((stripe, width), bf16),
            vmem((own, features), bf16),
            vmem((slots, features), bf16),
        ]
        + [dma((layers * chunks,))] * 6
        + [dma((chunks,))] * 8
        + [dma((line,))] * 2
        + [dma((bits + 1,))] * 4
        + [dma((line,))] * 2
        + [dma((bits,))] * 2,
        compiler_params=pltpu.CompilerParams(
            collective_id=0, has_side_effects=True, vmem_limit_bytes=60 * 2**20
        ),
        cost_estimate=pl.CostEstimate(flops=flops, bytes_accessed=flops // 256, transcendentals=0),
    )(state, norm_gain, win, wout)


def mix(n_dp, n_mp, *args):
    (patch_query, key_cache, value_cache, cache_len, patch_end, ended_index, pool_out, norm_gain, w_in, w_out) = args
    layers, block_cols, _, hidden_local = w_in.shape
    pieces = hidden_local // LANES
    win = w_in.reshape(layers, block_cols, 2, pieces, LANES).transpose(0, 3, 1, 2, 4)
    win = win.reshape(layers, pieces, block_cols, 2 * LANES)

    seq_rows = patch_query.shape[0]
    heads_width = key_cache.shape[2]
    place = lax.axis_index("mp")
    query_cols = lax.dynamic_slice_in_dim(patch_query, place * heads_width, heads_width, 1)
    attended = attend_local(query_cols, key_cache, value_cache, cache_len)
    picker = (ended_index[:, None] == jnp.arange(seq_rows, dtype=jnp.int32)[None, :]).astype(
        jnp.bfloat16
    )
    chosen = jnp.dot(picker, attended, preferred_element_type=jnp.float32).astype(jnp.bfloat16)
    partial_value = jnp.dot(chosen, pool_out, preferred_element_type=jnp.float32)
    pooled = own_rows_of_sum(partial_value.astype(jnp.bfloat16), n_mp)
    own = picker.shape[0] // n_mp
    reverse, bit = 0, 1
    while bit < n_mp:
        reverse = reverse * 2 + (place // bit) % 2
        bit *= 2
    own_picker = lax.dynamic_slice_in_dim(picker, reverse * own, own, 0)
    query_rows = jnp.dot(own_picker, patch_query, preferred_element_type=jnp.float32)
    state = run_layers(n_dp, n_mp, query_rows + pooled, norm_gain, win, w_out)
    placed = jnp.dot(picker.T, state, preferred_element_type=jnp.float32)
    return (placed * patch_end.astype(jnp.float32)[:, None]).astype(jnp.bfloat16)


def solution(mesh):
    in_specs = (
        P("dp", None),
        P("dp", None, "mp"),
        P("dp", None, "mp"),
        P("dp"),
        P("dp"),
        P("dp"),
        P("mp", None),
        P(),
        P(None, "dp", None, "mp"),
        P(None, "mp", "dp"),
    )
    out_specs = P("dp", None)
    def per_device(*args):
        return mix(mesh.shape["dp"], mesh.shape["mp"], *args)

    return jax.shard_map(
        per_device, mesh=mesh, in_specs=in_specs, out_specs=out_specs, check_vma=False
    )
```

```python
import functools

import jax
import jax.numpy as jnp
from jax import lax
from jax.experimental import pallas as pl
from jax.experimental.pallas import tpu as pltpu
from jax.sharding import PartitionSpec as P

HEAD_DIM = 128
LANES = 128
PARTS = 4
SKEW = 1
SKEW_HID = 1


norm_floor = 1e-05


def attend_local(query_cols, keys, values, lengths):
    seq_rows, patch_len, heads_width = keys.shape
    head_count = heads_width // HEAD_DIM
    query_heads = query_cols.reshape(seq_rows, head_count, HEAD_DIM)
    key_heads = keys.reshape(seq_rows, patch_len, head_count, HEAD_DIM)
    value_heads = values.reshape(seq_rows, patch_len, head_count, HEAD_DIM)
    scores = jnp.einsum(
        "shd,sphd->shp", query_heads, key_heads, preferred_element_type=jnp.float32
    ) * HEAD_DIM ** (-0.5)
    live_mask = jnp.arange(patch_len, dtype=jnp.int32)[None, None, :] < lengths[:, None, None]
    scores = jnp.where(live_mask, scores, jnp.float32(-1e30))
    top_score = jnp.max(scores, axis=2, keepdims=True)
    expo = jnp.where(live_mask, jnp.exp(scores - top_score), jnp.float32(0.0))
    weights = (expo / jnp.sum(expo, axis=2, keepdims=True)).astype(jnp.bfloat16)
    mixed = jnp.einsum("shp,sphd->shd", weights, value_heads, preferred_element_type=jnp.float32)
    return mixed.astype(jnp.bfloat16).reshape(seq_rows, heads_width)


def swap(value, axis, size, bit):
    return lax.ppermute(value, axis, [(i, i ^ bit) for i in range(size)])


def own_rows_of_sum(value, size):
    place = lax.axis_index("mp")
    bit = 1
    total = value.astype(jnp.float32)
    while bit < size:
        half = total.shape[0] // 2
        low = (place // bit) % 2
        kept = lax.dynamic_slice_in_dim(total, low * half, half, 0)
        given = lax.dynamic_slice_in_dim(total, (1 - low) * half, half, 0).astype(jnp.bfloat16)
        total = kept + swap(given, "mp", size, bit).astype(jnp.float32)
        bit *= 2
    return total


def layers_kernel(
    n_dp, n_mp, state_in, gain_ref, win_ref, wout_ref, out_ref,
    state, normed, feats, acc, w_up, w_down, right_buf, left_buf, right_hid, left_hid,
    give, got, share, back, final,
    wl_sem, ws_sem, wr_sem, ol_sem, os_sem, or_sem,
    rs_sem, rr_sem, ls_sem, lr_sem, hrs_sem, hrr_sem, hls_sem, hlr_sem,
    az_s, az_r, ag_s, ag_r, dd_s, dd_r, dz_s, dz_r, ff_s, ff_r,
):
    layers, chunks, _, full_width, _ = w_up.shape
    line = n_dp // 2
    bits = n_mp.bit_length() - 1
    block_cols = full_width // 2
    own = state.shape[0]
    stripe = line * own
    half_rows = right_buf.shape[1]
    dp, mp = lax.axis_index("dp"), lax.axis_index("mp")
    z, y = dp // 2, dp % 2
    top = line - 1
    reverse = 0
    for i in range(bits):
        reverse = reverse + ((mp // (1 << i)) % 2) * (1 << (bits - 1 - i))
    block = reverse * 2 + y

    def flip(value, bit):
        return value + bit - 2 * bit * ((value // bit) % 2)

    def partner(t):
        if t == 0:
            return (dp + 1 - 2 * y, mp)
        return (dp, flip(mp, 1 << (bits - t)))

    def at_line(other):
        return (other * 2 + y, mp)

    def send(src, dst, s_sem, r_sem, device):
        return pltpu.make_async_remote_copy(
            src_ref=src, dst_ref=dst, send_sem=s_sem, recv_sem=r_sem,
            device_id=device, device_id_type=pl.DeviceIdType.MESH,
        )

    barrier = pltpu.get_barrier_semaphore()
    for d in range(1, line):
        pl.semaphore_signal(
            barrier, inc=1, device_id=at_line((z + d) % line), device_id_type=pl.DeviceIdType.MESH
        )
    for t in range(bits + 1):
        pl.semaphore_signal(barrier, inc=1, device_id=partner(t), device_id_type=pl.DeviceIdType.MESH)
    pl.semaphore_wait(barrier, line - 1 + bits + 1)

    pieces = layers * chunks
    part_cols = full_width // PARTS

    def own_up(l, q):
        return pltpu.make_async_copy(
            win_ref.at[l, :, :, pl.ds(pl.multiple_of((y * chunks + q) * LANES, LANES), LANES)],
            w_up.at[l, q, :, pl.ds(y * block_cols, block_cols), :],
            wl_sem.at[l * chunks + q],
        )

    def own_down(l, q):
        return pltpu.make_async_copy(
            wout_ref.at[l, pl.ds((y * chunks + q) * LANES, LANES), :],
            w_down.at[l, q, y],
            ol_sem.at[l * chunks + q],
        )

    def give_up(l, q):
        return send(
            win_ref.at[l, :, :, pl.ds(pl.multiple_of(((1 - y) * chunks + q) * LANES, LANES), LANES)],
            w_up.at[l, q, :, pl.ds(y * block_cols, block_cols), :],
            ws_sem.at[l * chunks + q], wr_sem.at[l * chunks + q], partner(0),
        )

    def give_down(l, q):
        return send(
            wout_ref.at[l, pl.ds(((1 - y) * chunks + q) * LANES, LANES), :],
            w_down.at[l, q, y],
            os_sem.at[l * chunks + q], or_sem.at[l * chunks + q], partner(0),
        )

    def issue_up(piece):
        @pl.when(piece < pieces)
        def _():
            give_up(piece // chunks, piece % chunks).start()

    def issue_down(piece):
        @pl.when(piece < pieces)
        def _():
            give_down(piece // chunks, piece % chunks).start()

    def start_own(piece, carry):
        own_up(piece // chunks, piece % chunks).start()
        own_down(piece // chunks, piece % chunks).start()
        return carry

    issue_up(jnp.int32(0))
    lax.fori_loop(0, pieces, start_own, 0)

    state[...] = state_in[...]
    first_use = SKEW * jnp.minimum(z, top - z)
    first_down = SKEW_HID * jnp.minimum(z, top - z) + SKEW * top + 1
    steps = chunks + (SKEW + SKEW_HID) * top + 1
    def one_layer(l, carry):
        value = state[...]
        scale = lax.rsqrt(jnp.mean(value * value, axis=1, keepdims=True) + norm_floor)
        normed[...] = (value * scale * gain_ref[pl.ds(l, 1), :]).astype(jnp.bfloat16)
        mine = block * stripe + z * own
        next_up, next_down = l * (chunks + 4), l * (chunks + 1)

        def spread(c, d):
            other = (z + d) % line
            return send(
                normed.at[
                    :, pl.ds(pl.multiple_of(other * full_width + c * part_cols, LANES), part_cols)
                ],
                feats.at[
                    pl.ds(pl.multiple_of(mine, own), own), pl.ds(c * part_cols, part_cols)
                ],
                az_s.at[c * line + d], az_r.at[c * line + d], at_line(other),
            )

        def gather(c, t):
            rows = stripe << t
            start = pl.multiple_of((block // (1 << t)) * rows, stripe)
            ref = feats.at[pl.ds(start, rows), pl.ds(c * part_cols, part_cols)]
            at = c * (bits + 1) + t
            return send(ref, ref, ag_s.at[at], ag_r.at[at], partner(t))

        for c in range(PARTS):
            for d in range(1, line):
                spread(c, d).start()
        feats[pl.ds(pl.multiple_of(mine, own), own), :] = normed[
            :, pl.ds(pl.multiple_of(z * full_width, LANES), full_width)
        ]
        for t in range(bits + 1):
            for c in range(PARTS):
                if t == 0:
                    for d in range(1, line):
                        spread(c, d).wait_recv()
                else:
                    gather(c, t - 1).wait_recv()
                gather(c, t).start()
            if t == 0:
                for i in range(1, 4):
                    issue_up(next_up + i)
        for c in range(PARTS):
            gather(c, bits).wait_recv()
        for c in range(PARTS):
            for d in range(1, line):
                spread(c, d).wait_send()
            for t in range(bits + 1):
                gather(c, t).wait_send()

        acc[...] = jnp.zeros_like(acc)

        def hidden_of(total):
            gate, up = total[:, :LANES], total[:, LANES:]
            return (gate / (1.0 + jnp.exp(-gate)) * up).astype(jnp.bfloat16)

        def chain(q, row0, first, last, to_next, to_prev, buf, hid, s_s, s_r, h_s, h_r):
            both = jnp.concatenate([w_up[l, q, 0], w_up[l, q, 1]], axis=1)
            part = jnp.dot(
                feats[row0 : row0 + half_rows, :], both, preferred_element_type=jnp.float32
            )

            @pl.when(z == first)
            def _():
                buf[q] = part.astype(jnp.bfloat16)

            @pl.when(z != first)
            def _():
                send(buf.at[q], buf.at[q], s_s.at[q], s_r.at[q], at_line(to_next)).wait_recv()

            @pl.when(jnp.logical_and(z != first, z != last))
            def _():
                buf[q] = (part + buf[q].astype(jnp.float32)).astype(jnp.bfloat16)

            @pl.when(z == last)
            def _():
                hid[q] = hidden_of(part + buf[q].astype(jnp.float32))
                send(hid.at[q], hid.at[q], h_s.at[q], h_r.at[q], at_line(to_prev)).start()

            @pl.when(z != last)
            def _():
                send(buf.at[q], buf.at[q], s_s.at[q], s_r.at[q], at_line(to_next)).start()

        def pass_on(q, first, last, to_prev, hid, h_s, h_r):
            @pl.when(z != last)
            def _():
                send(hid.at[q], hid.at[q], h_s.at[q], h_r.at[q], at_line(to_prev)).wait_recv()

            @pl.when(jnp.logical_and(z != last, z != first))
            def _():
                send(hid.at[q], hid.at[q], h_s.at[q], h_r.at[q], at_line(to_prev)).start()

        def down(q, row0, hid):
            for c in range(2):
                cols = slice(c * block_cols, (c + 1) * block_cols)
                acc[row0 : row0 + half_rows, cols] += jnp.dot(
                    hid[q], w_down[l, q, c], preferred_element_type=jnp.float32
                )

        nxt, prv = jnp.minimum(z + 1, top), jnp.maximum(z - 1, 0)

        def within(q):
            return jnp.logical_and(q >= 0, q < chunks)

        def one_step(s, inner):
            qw = s - first_use

            @pl.when(within(qw))
            def _():
                own_up(l, qw).wait()
                give_up(l, qw).wait_recv()

            qd = s - first_down

            @pl.when(within(qd))
            def _():
                own_down(l, qd).wait()
                give_down(l, qd).wait_recv()

            qr = s - SKEW * z

            @pl.when(within(qr))
            def _():
                chain(qr, 0, 0, top, nxt, prv, right_buf, right_hid,
                      rs_sem, rr_sem, hrs_sem, hrr_sem)

            ql = s - SKEW * (top - z)

            @pl.when(within(ql))
            def _():
                chain(ql, half_rows, top, 0, prv, nxt, left_buf, left_hid,
                      ls_sem, lr_sem, hls_sem, hlr_sem)

            hr = s - (SKEW * top + 1) - SKEW_HID * (top - z)

            @pl.when(within(hr))
            def _():
                pass_on(hr, 0, top, prv, right_hid, hrs_sem, hrr_sem)

            hl = s - (SKEW * top + 1) - SKEW_HID * z

            @pl.when(within(hl))
            def _():
                pass_on(hl, top, 0, nxt, left_hid, hls_sem, hlr_sem)

            @pl.when(s < chunks)
            def _():
                issue_up(next_up + 4 + s)
                issue_down(next_down + s)

            @pl.when(within(hr))
            def _():
                down(hr, 0, right_hid)

            @pl.when(within(hl))
            def _():
                down(hl, half_rows, left_hid)

            return inner

        lax.fori_loop(0, steps, one_step, 0)

        def drain(q, inner):
            @pl.when(z != top)
            def _():
                send(right_buf.at[q], right_buf.at[q], rs_sem.at[q], rr_sem.at[q],
                     at_line(nxt)).wait_send()

            @pl.when(z != 0)
            def _():
                send(left_buf.at[q], left_buf.at[q], ls_sem.at[q], lr_sem.at[q],
                     at_line(prv)).wait_send()

            @pl.when(z != 0)
            def _():
                send(right_hid.at[q], right_hid.at[q], hrs_sem.at[q], hrr_sem.at[q],
                     at_line(prv)).wait_send()

            @pl.when(z != top)
            def _():
                send(left_hid.at[q], left_hid.at[q], hls_sem.at[q], hlr_sem.at[q],
                     at_line(nxt)).wait_send()

            return inner

        lax.fori_loop(0, chunks, drain, 0)

        def side(t):
            return (block // (1 << t)) % 2

        def halve(c, t):
            rows = stripe << t
            at = stripe * ((1 << t) - 1)
            cols = pl.ds(c * part_cols, part_cols)
            number = c * (bits + 1) + t
            return send(
                give.at[pl.ds(at, rows), cols], got.at[pl.ds(at, rows), cols],
                dd_s.at[number], dd_r.at[number], partner(t),
            )

        def start_halve(c, t):
            rows = stripe << t
            at = stripe * ((1 << t) - 1)
            cols = slice(c * part_cols, (c + 1) * part_cols)
            there = pl.multiple_of((block // (1 << t) + 1 - 2 * side(t)) * rows, stripe)
            give[at : at + rows, cols] = acc[pl.ds(there, rows), cols].astype(jnp.bfloat16)
            halve(c, t).start()

        def bring(c, d):
            other = (z + d) % line
            return send(
                share.at[
                    pl.ds(pl.multiple_of(other * own, own), own), pl.ds(c * part_cols, part_cols)
                ],
                back.at[
                    :, pl.ds(pl.multiple_of(z * full_width + c * part_cols, LANES), part_cols)
                ],
                dz_s.at[c * line + d], dz_r.at[c * line + d], at_line(other),
            )

        for c in range(PARTS):
            start_halve(c, bits)
        for t in range(bits, -1, -1):
            rows = stripe << t
            at = stripe * ((1 << t) - 1)
            here = pl.multiple_of((block // (1 << t)) * rows, stripe)
            for c in range(PARTS):
                cols = slice(c * part_cols, (c + 1) * part_cols)
                halve(c, t).wait_recv()
                acc[pl.ds(here, rows), cols] += got[at : at + rows, cols].astype(jnp.float32)
                if t > 0:
                    start_halve(c, t - 1)
                else:
                    share[:, cols] = acc[pl.ds(here, rows), cols].astype(jnp.bfloat16)
                    for d in range(1, line):
                        bring(c, d).start()
            if t == 1:
                issue_up(next_up + chunks + 4)
                issue_down(next_down + chunks)
        columns = pl.ds(pl.multiple_of(z * full_width, LANES), full_width)
        back[:, columns] = share[pl.ds(pl.multiple_of(z * own, own), own), :]
        for c in range(PARTS):
            for d in range(1, line):
                bring(c, d).wait()
            for t in range(bits + 1):
                halve(c, t).wait_send()
        state[...] += back[...].astype(jnp.float32)
        return carry

    lax.fori_loop(0, layers, one_layer, 0)

    def drain_weights(piece, carry):
        give_up(piece // chunks, piece % chunks).wait_send()
        give_down(piece // chunks, piece % chunks).wait_send()
        return carry

    lax.fori_loop(0, pieces, drain_weights, 0)

    final[pl.ds(pl.multiple_of(reverse * own, own), own), :] = state[...].astype(jnp.bfloat16)
    for t in range(bits):
        rows = own << t
        ref = final.at[pl.ds(pl.multiple_of((reverse // (1 << t)) * rows, own), rows), :]
        step = send(ref, ref, ff_s.at[t], ff_r.at[t], partner(t + 1))
        step.start()
        step.wait()
    out_ref[...] = final[...]


def run_layers(n_dp, n_mp, state, norm_gain, win, wout):
    layers, _, block_cols, hidden_local = win.shape
    own, features = state.shape
    chunks = hidden_local // 2 // LANES
    line = n_dp // 2
    bits = n_mp.bit_length() - 1
    width = 2 * block_cols
    rows = own * line * 2 * n_mp
    half = rows // 2
    slots = own * n_mp
    dma = pltpu.SemaphoreType.DMA
    vmem = pltpu.VMEM
    bf16, f32 = jnp.bfloat16, jnp.float32
    stripe = own * line
    passing = stripe * (2 * n_mp - 1)
    flops = 2 * layers * rows * chunks * LANES * 3 * width
    return pl.pallas_call(
        functools.partial(layers_kernel, n_dp, n_mp),
        name="global_layers",
        out_shape=jax.ShapeDtypeStruct((slots, features), bf16),
        in_specs=[
            pl.BlockSpec(memory_space=pltpu.VMEM),
            pl.BlockSpec(memory_space=pltpu.VMEM),
            pl.BlockSpec(memory_space=pl.ANY),
            pl.BlockSpec(memory_space=pl.ANY),
        ],
        out_specs=pl.BlockSpec(memory_space=pltpu.VMEM),
        scratch_shapes=[
            vmem((own, features), f32),
            vmem((own, features), bf16),
            vmem((rows, width), bf16),
            vmem((rows, width), f32),
            vmem((layers, chunks, 2, width, LANES), bf16),
            vmem((layers, chunks, 2, LANES, block_cols), bf16),
            vmem((chunks, half, 2 * LANES), bf16),
            vmem((chunks, half, 2 * LANES), bf16),
            vmem((chunks, half, LANES), bf16),
            vmem((chunks, half, LANES), bf16),
            vmem((passing, width), bf16),
            vmem((passing, width), bf16),
            vmem((stripe, width), bf16),
            vmem((own, features), bf16),
            vmem((slots, features), bf16),
        ]
        + [dma((layers * chunks,))] * 6
        + [dma((chunks,))] * 8
        + [dma((PARTS * line,))] * 2
        + [dma((PARTS * (bits + 1),))] * 4
        + [dma((PARTS * line,))] * 2
        + [dma((bits,))] * 2,
        compiler_params=pltpu.CompilerParams(
            collective_id=0, has_side_effects=True, vmem_limit_bytes=60 * 2**20
        ),
        cost_estimate=pl.CostEstimate(flops=flops, bytes_accessed=flops // 256, transcendentals=0),
    )(state, norm_gain, win, wout)


def mix(n_dp, n_mp, *args):
    (patch_query, key_cache, value_cache, cache_len, patch_end, ended_index, pool_out, norm_gain, w_in, w_out) = args
    layers, block_cols, _, hidden_local = w_in.shape
    win = w_in.transpose(0, 2, 1, 3)

    seq_rows = patch_query.shape[0]
    heads_width = key_cache.shape[2]
    place = lax.axis_index("mp")
    query_cols = lax.dynamic_slice_in_dim(patch_query, place * heads_width, heads_width, 1)
    attended = attend_local(query_cols, key_cache, value_cache, cache_len)
    picker = (ended_index[:, None] == jnp.arange(seq_rows, dtype=jnp.int32)[None, :]).astype(
        jnp.bfloat16
    )
    chosen = jnp.dot(picker, attended, preferred_element_type=jnp.float32).astype(jnp.bfloat16)
    partial_value = jnp.dot(chosen, pool_out, preferred_element_type=jnp.float32)
    pooled = own_rows_of_sum(partial_value.astype(jnp.bfloat16), n_mp)
    own = picker.shape[0] // n_mp
    reverse, bit = 0, 1
    while bit < n_mp:
        reverse = reverse * 2 + (place // bit) % 2
        bit *= 2
    own_picker = lax.dynamic_slice_in_dim(picker, reverse * own, own, 0)
    query_rows = jnp.dot(own_picker, patch_query, preferred_element_type=jnp.float32)
    state = run_layers(n_dp, n_mp, query_rows + pooled, norm_gain, win, w_out)
    placed = jnp.dot(picker.T, state, preferred_element_type=jnp.float32)
    return (placed * patch_end.astype(jnp.float32)[:, None]).astype(jnp.bfloat16)


def solution(mesh):
    in_specs = (
        P("dp", None),
        P("dp", None, "mp"),
        P("dp", None, "mp"),
        P("dp"),
        P("dp"),
        P("dp"),
        P("mp", None),
        P(),
        P(None, "dp", None, "mp"),
        P(None, "mp", "dp"),
    )
    out_specs = P("dp", None)
    def per_device(*args):
        return mix(mesh.shape["dp"], mesh.shape["mp"], *args)

    return jax.shard_map(
        per_device, mesh=mesh, in_specs=in_specs, out_specs=out_specs, check_vma=False
    )
```

```python
import functools

import jax
import jax.numpy as jnp
from jax import lax
from jax.experimental import pallas as pl
from jax.experimental.pallas import tpu as pltpu
from jax.sharding import PartitionSpec as P

HEAD_DIM = 128
LANES = 128
PARTS = 4
SIZES = (20, 23, 26, 32)
SKEW = 1
SKEW_HID = 1


norm_floor = 1e-05


def attend_local(query_cols, keys, values, lengths):
    seq_rows, patch_len, heads_width = keys.shape
    head_count = heads_width // HEAD_DIM
    query_heads = query_cols.reshape(seq_rows, head_count, HEAD_DIM)
    key_heads = keys.reshape(seq_rows, patch_len, head_count, HEAD_DIM)
    value_heads = values.reshape(seq_rows, patch_len, head_count, HEAD_DIM)
    scores = jnp.einsum(
        "shd,sphd->shp", query_heads, key_heads, preferred_element_type=jnp.float32
    ) * HEAD_DIM ** (-0.5)
    live_mask = jnp.arange(patch_len, dtype=jnp.int32)[None, None, :] < lengths[:, None, None]
    scores = jnp.where(live_mask, scores, jnp.float32(-1e30))
    top_score = jnp.max(scores, axis=2, keepdims=True)
    expo = jnp.where(live_mask, jnp.exp(scores - top_score), jnp.float32(0.0))
    weights = (expo / jnp.sum(expo, axis=2, keepdims=True)).astype(jnp.bfloat16)
    mixed = jnp.einsum("shp,sphd->shd", weights, value_heads, preferred_element_type=jnp.float32)
    return mixed.astype(jnp.bfloat16).reshape(seq_rows, heads_width)


def swap(value, axis, size, bit):
    return lax.ppermute(value, axis, [(i, i ^ bit) for i in range(size)])


def own_rows_of_sum(value, size):
    place = lax.axis_index("mp")
    bit = 1
    total = value.astype(jnp.float32)
    while bit < size:
        half = total.shape[0] // 2
        low = (place // bit) % 2
        kept = lax.dynamic_slice_in_dim(total, low * half, half, 0)
        given = lax.dynamic_slice_in_dim(total, (1 - low) * half, half, 0).astype(jnp.bfloat16)
        total = kept + swap(given, "mp", size, bit).astype(jnp.float32)
        bit *= 2
    return total


def layers_kernel(
    n_dp, n_mp, packed, *refs
):
    (state_in, gain_ref, win_ref, wout_ref), refs = refs[:4], refs[4:]
    if packed:
        (pick, lay), refs = refs[:2], refs[2:]
    (out_ref, state, normed, feats, acc, w_up, w_down, right_buf, left_buf, right_hid, left_hid,
     give, got, share, back, final), refs = refs[:16], refs[16:]
    if packed:
        (live, total), refs = refs[:2], refs[2:]
    else:
        live, total = feats, acc
    (
    wl_sem, ws_sem, wr_sem, ol_sem, os_sem, or_sem,
    rs_sem, rr_sem, ls_sem, lr_sem, hrs_sem, hrr_sem, hls_sem, hlr_sem,
    az_s, az_r, ag_s, ag_r, dd_s, dd_r, dz_s, dz_r, ff_s, ff_r,
    ) = refs
    layers, chunks, _, full_width, _ = w_up.shape
    line = n_dp // 2
    bits = n_mp.bit_length() - 1
    block_cols = full_width // 2
    own = state.shape[0]
    stripe = line * own
    half_rows = right_buf.shape[1]
    dp, mp = lax.axis_index("dp"), lax.axis_index("mp")
    z, y = dp // 2, dp % 2
    top = line - 1
    reverse = 0
    for i in range(bits):
        reverse = reverse + ((mp // (1 << i)) % 2) * (1 << (bits - 1 - i))
    block = reverse * 2 + y

    def flip(value, bit):
        return value + bit - 2 * bit * ((value // bit) % 2)

    def partner(t):
        if t == 0:
            return (dp + 1 - 2 * y, mp)
        return (dp, flip(mp, 1 << (bits - t)))

    def at_line(other):
        return (other * 2 + y, mp)

    def send(src, dst, s_sem, r_sem, device):
        return pltpu.make_async_remote_copy(
            src_ref=src, dst_ref=dst, send_sem=s_sem, recv_sem=r_sem,
            device_id=device, device_id_type=pl.DeviceIdType.MESH,
        )

    barrier = pltpu.get_barrier_semaphore()
    for d in range(1, line):
        pl.semaphore_signal(
            barrier, inc=1, device_id=at_line((z + d) % line), device_id_type=pl.DeviceIdType.MESH
        )
    for t in range(bits + 1):
        pl.semaphore_signal(barrier, inc=1, device_id=partner(t), device_id_type=pl.DeviceIdType.MESH)
    pl.semaphore_wait(barrier, line - 1 + bits + 1)

    pieces = layers * chunks
    part_cols = full_width // PARTS

    def own_up(l, q):
        return pltpu.make_async_copy(
            win_ref.at[l, :, :, pl.ds(pl.multiple_of((y * chunks + q) * LANES, LANES), LANES)],
            w_up.at[l, q, :, pl.ds(y * block_cols, block_cols), :],
            wl_sem.at[l * chunks + q],
        )

    def own_down(l, q):
        return pltpu.make_async_copy(
            wout_ref.at[l, pl.ds((y * chunks + q) * LANES, LANES), :],
            w_down.at[l, q, y],
            ol_sem.at[l * chunks + q],
        )

    def give_up(l, q):
        return send(
            win_ref.at[l, :, :, pl.ds(pl.multiple_of(((1 - y) * chunks + q) * LANES, LANES), LANES)],
            w_up.at[l, q, :, pl.ds(y * block_cols, block_cols), :],
            ws_sem.at[l * chunks + q], wr_sem.at[l * chunks + q], partner(0),
        )

    def give_down(l, q):
        return send(
            wout_ref.at[l, pl.ds(((1 - y) * chunks + q) * LANES, LANES), :],
            w_down.at[l, q, y],
            os_sem.at[l * chunks + q], or_sem.at[l * chunks + q], partner(0),
        )

    def issue_up(piece):
        @pl.when(piece < pieces)
        def _():
            give_up(piece // chunks, piece % chunks).start()

    def issue_down(piece):
        @pl.when(piece < pieces)
        def _():
            give_down(piece // chunks, piece % chunks).start()

    def start_own(piece, carry):
        own_up(piece // chunks, piece % chunks).start()
        own_down(piece // chunks, piece % chunks).start()
        return carry

    issue_up(jnp.int32(0))
    lax.fori_loop(0, pieces, start_own, 0)

    state[...] = state_in[...]
    first_use = SKEW * jnp.minimum(z, top - z)
    first_down = SKEW_HID * jnp.minimum(z, top - z) + SKEW * top + 1
    steps = chunks + (SKEW + SKEW_HID) * top + 1
    def one_layer(l, carry):
        value = state[...]
        scale = lax.rsqrt(jnp.mean(value * value, axis=1, keepdims=True) + norm_floor)
        normed[...] = (value * scale * gain_ref[pl.ds(l, 1), :]).astype(jnp.bfloat16)
        mine = block * stripe + z * own
        next_up, next_down = l * (chunks + 4), l * (chunks + 1)

        def spread(c, d):
            other = (z + d) % line
            return send(
                normed.at[
                    :, pl.ds(pl.multiple_of(other * full_width + c * part_cols, LANES), part_cols)
                ],
                feats.at[
                    pl.ds(pl.multiple_of(mine, own), own), pl.ds(c * part_cols, part_cols)
                ],
                az_s.at[c * line + d], az_r.at[c * line + d], at_line(other),
            )

        def gather(c, t):
            rows = stripe << t
            start = pl.multiple_of((block // (1 << t)) * rows, stripe)
            ref = feats.at[
                pl.ds(start, rows), pl.ds(pl.multiple_of(c * part_cols, LANES), part_cols)
            ]
            at = c * (bits + 1) + t
            return send(ref, ref, ag_s.at[at], ag_r.at[at], partner(t))

        for c in range(PARTS):
            for d in range(1, line):
                spread(c, d).start()
        feats[pl.ds(pl.multiple_of(mine, own), own), :] = normed[
            :, pl.ds(pl.multiple_of(z * full_width, LANES), full_width)
        ]
        for t in range(bits + 1):
            for c in range(PARTS):
                if t == 0:
                    for d in range(1, line):
                        spread(c, d).wait_recv()
                else:
                    gather(c, t - 1).wait_recv()
                gather(c, t).start()
            if t == 0:
                for i in range(1, 4):
                    issue_up(next_up + i)

        def arrived(c, inner):
            gather(c, bits).wait_recv()
            if packed:
                cols = pl.ds(pl.multiple_of(c * part_cols, LANES), part_cols)
                live[:, cols] = jnp.dot(
                    pick[...], feats[:, cols], preferred_element_type=jnp.float32
                ).astype(jnp.bfloat16)
            return inner

        lax.fori_loop(0, PARTS, arrived, 0)
        for c in range(PARTS):
            for d in range(1, line):
                spread(c, d).wait_send()
            for t in range(bits + 1):
                gather(c, t).wait_send()

        total[...] = jnp.zeros_like(total)

        def hidden_of(both):
            gate, up = both[:, :LANES], both[:, LANES:]
            return (gate / (1.0 + jnp.exp(-gate)) * up).astype(jnp.bfloat16)

        def chain(q, row0, first, last, to_next, to_prev, buf, hid, s_s, s_r, h_s, h_r):
            both = jnp.concatenate([w_up[l, q, 0], w_up[l, q, 1]], axis=1)
            part = jnp.dot(
                live[row0 : row0 + half_rows, :], both, preferred_element_type=jnp.float32
            )

            @pl.when(z == first)
            def _():
                buf[q] = part.astype(jnp.bfloat16)

            @pl.when(z != first)
            def _():
                send(buf.at[q], buf.at[q], s_s.at[q], s_r.at[q], at_line(to_next)).wait_recv()

            @pl.when(jnp.logical_and(z != first, z != last))
            def _():
                buf[q] = (part + buf[q].astype(jnp.float32)).astype(jnp.bfloat16)

            @pl.when(z == last)
            def _():
                hid[q] = hidden_of(part + buf[q].astype(jnp.float32))
                send(hid.at[q], hid.at[q], h_s.at[q], h_r.at[q], at_line(to_prev)).start()

            @pl.when(z != last)
            def _():
                send(buf.at[q], buf.at[q], s_s.at[q], s_r.at[q], at_line(to_next)).start()

        def pass_on(q, first, last, to_prev, hid, h_s, h_r):
            @pl.when(z != last)
            def _():
                send(hid.at[q], hid.at[q], h_s.at[q], h_r.at[q], at_line(to_prev)).wait_recv()

            @pl.when(jnp.logical_and(z != last, z != first))
            def _():
                send(hid.at[q], hid.at[q], h_s.at[q], h_r.at[q], at_line(to_prev)).start()

        def down(q, row0, hid):
            for c in range(2):
                cols = slice(c * block_cols, (c + 1) * block_cols)
                total[row0 : row0 + half_rows, cols] += jnp.dot(
                    hid[q], w_down[l, q, c], preferred_element_type=jnp.float32
                )

        nxt, prv = jnp.minimum(z + 1, top), jnp.maximum(z - 1, 0)

        def within(q):
            return jnp.logical_and(q >= 0, q < chunks)

        def one_step(s, inner):
            qw = s - first_use

            @pl.when(within(qw))
            def _():
                own_up(l, qw).wait()
                give_up(l, qw).wait_recv()

            qd = s - first_down

            @pl.when(within(qd))
            def _():
                own_down(l, qd).wait()
                give_down(l, qd).wait_recv()

            qr = s - SKEW * z

            @pl.when(within(qr))
            def _():
                chain(qr, 0, 0, top, nxt, prv, right_buf, right_hid,
                      rs_sem, rr_sem, hrs_sem, hrr_sem)

            ql = s - SKEW * (top - z)

            @pl.when(within(ql))
            def _():
                chain(ql, half_rows, top, 0, prv, nxt, left_buf, left_hid,
                      ls_sem, lr_sem, hls_sem, hlr_sem)

            hr = s - (SKEW * top + 1) - SKEW_HID * (top - z)

            @pl.when(within(hr))
            def _():
                pass_on(hr, 0, top, prv, right_hid, hrs_sem, hrr_sem)

            hl = s - (SKEW * top + 1) - SKEW_HID * z

            @pl.when(within(hl))
            def _():
                pass_on(hl, top, 0, nxt, left_hid, hls_sem, hlr_sem)

            @pl.when(s < chunks)
            def _():
                issue_up(next_up + 4 + s)
                issue_down(next_down + s)

            @pl.when(within(hr))
            def _():
                down(hr, 0, right_hid)

            @pl.when(within(hl))
            def _():
                down(hl, half_rows, left_hid)

            return inner

        lax.fori_loop(0, steps, one_step, 0)

        def drain(q, inner):
            @pl.when(z != top)
            def _():
                send(right_buf.at[q], right_buf.at[q], rs_sem.at[q], rr_sem.at[q],
                     at_line(nxt)).wait_send()

            @pl.when(z != 0)
            def _():
                send(left_buf.at[q], left_buf.at[q], ls_sem.at[q], lr_sem.at[q],
                     at_line(prv)).wait_send()

            @pl.when(z != 0)
            def _():
                send(right_hid.at[q], right_hid.at[q], hrs_sem.at[q], hrr_sem.at[q],
                     at_line(prv)).wait_send()

            @pl.when(z != top)
            def _():
                send(left_hid.at[q], left_hid.at[q], hls_sem.at[q], hlr_sem.at[q],
                     at_line(nxt)).wait_send()

            return inner

        lax.fori_loop(0, chunks, drain, 0)

        def side(t):
            return (block // (1 << t)) % 2

        def halve(c, t):
            rows = stripe << t
            at = stripe * ((1 << t) - 1)
            cols = pl.ds(pl.multiple_of(c * part_cols, LANES), part_cols)
            number = c * (bits + 1) + t
            return send(
                give.at[pl.ds(at, rows), cols], got.at[pl.ds(at, rows), cols],
                dd_s.at[number], dd_r.at[number], partner(t),
            )

        def start_halve(c, t):
            rows = stripe << t
            at = stripe * ((1 << t) - 1)
            cols = pl.ds(pl.multiple_of(c * part_cols, LANES), part_cols)
            there = pl.multiple_of((block // (1 << t) + 1 - 2 * side(t)) * rows, stripe)
            give[pl.ds(at, rows), cols] = acc[pl.ds(there, rows), cols].astype(jnp.bfloat16)
            halve(c, t).start()

        def bring(c, d):
            other = (z + d) % line
            return send(
                share.at[
                    pl.ds(pl.multiple_of(other * own, own), own), pl.ds(c * part_cols, part_cols)
                ],
                back.at[
                    :, pl.ds(pl.multiple_of(z * full_width + c * part_cols, LANES), part_cols)
                ],
                dz_s.at[c * line + d], dz_r.at[c * line + d], at_line(other),
            )

        def leave(c, inner):
            if packed:
                cols = pl.ds(pl.multiple_of(c * part_cols, LANES), part_cols)
                acc[:, cols] = jnp.dot(
                    lay[...], total[:, cols].astype(jnp.bfloat16), preferred_element_type=jnp.float32
                )
            start_halve(c, bits)
            return inner

        lax.fori_loop(0, PARTS, leave, 0)
        for t in range(bits, -1, -1):
            rows = stripe << t
            at = stripe * ((1 << t) - 1)
            here = pl.multiple_of((block // (1 << t)) * rows, stripe)
            for c in range(PARTS):
                cols = slice(c * part_cols, (c + 1) * part_cols)
                halve(c, t).wait_recv()
                acc[pl.ds(here, rows), cols] += got[at : at + rows, cols].astype(jnp.float32)
                if t > 0:
                    start_halve(c, t - 1)
                else:
                    share[:, cols] = acc[pl.ds(here, rows), cols].astype(jnp.bfloat16)
                    for d in range(1, line):
                        bring(c, d).start()
            if t == 1:
                issue_up(next_up + chunks + 4)
                issue_down(next_down + chunks)
        columns = pl.ds(pl.multiple_of(z * full_width, LANES), full_width)
        back[:, columns] = share[pl.ds(pl.multiple_of(z * own, own), own), :]
        for c in range(PARTS):
            for d in range(1, line):
                bring(c, d).wait()
            for t in range(bits + 1):
                halve(c, t).wait_send()
        state[...] += back[...].astype(jnp.float32)
        return carry

    lax.fori_loop(0, layers, one_layer, 0)

    def drain_weights(piece, carry):
        give_up(piece // chunks, piece % chunks).wait_send()
        give_down(piece // chunks, piece % chunks).wait_send()
        return carry

    lax.fori_loop(0, pieces, drain_weights, 0)

    final[pl.ds(pl.multiple_of(reverse * own, own), own), :] = state[...].astype(jnp.bfloat16)
    for t in range(bits):
        rows = own << t
        ref = final.at[pl.ds(pl.multiple_of((reverse // (1 << t)) * rows, own), rows), :]
        step = send(ref, ref, ff_s.at[t], ff_r.at[t], partner(t + 1))
        step.start()
        step.wait()
    out_ref[...] = final[...]


def run_layers(n_dp, n_mp, number, size, state, norm_gain, win, wout, place):
    layers, _, block_cols, hidden_local = win.shape
    own, features = state.shape
    chunks = hidden_local // 2 // LANES
    line = n_dp // 2
    bits = n_mp.bit_length() - 1
    width = 2 * block_cols
    rows = own * line * 2 * n_mp
    half = size // 2
    packed = size < rows
    slots = own * n_mp
    dma = pltpu.SemaphoreType.DMA
    vmem = pltpu.VMEM
    bf16, f32 = jnp.bfloat16, jnp.float32
    stripe = own * line
    passing = stripe * (2 * n_mp - 1)
    flops = 2 * layers * size * chunks * LANES * 3 * width
    tables, extra = [], []
    if packed:
        target = jnp.arange(size, dtype=jnp.int32)
        tables = [
            (target[:, None] == place[None, :]).astype(bf16),
            (place[:, None] == target[None, :]).astype(bf16),
        ]
        extra = [vmem((size, width), bf16), vmem((size, width), f32)]
    return pl.pallas_call(
        functools.partial(layers_kernel, n_dp, n_mp, packed),
        name="global_layers_%d" % number,
        out_shape=jax.ShapeDtypeStruct((slots, features), bf16),
        in_specs=[
            pl.BlockSpec(memory_space=pltpu.VMEM),
            pl.BlockSpec(memory_space=pltpu.VMEM),
            pl.BlockSpec(memory_space=pl.ANY),
            pl.BlockSpec(memory_space=pl.ANY),
        ]
        + [pl.BlockSpec(memory_space=pltpu.VMEM)] * len(tables),
        out_specs=pl.BlockSpec(memory_space=pltpu.VMEM),
        scratch_shapes=[
            vmem((own, features), f32),
            vmem((own, features), bf16),
            vmem((rows, width), bf16),
            vmem((rows, width), f32),
            vmem((layers, chunks, 2, width, LANES), bf16),
            vmem((layers, chunks, 2, LANES, block_cols), bf16),
            vmem((chunks, half, 2 * LANES), bf16),
            vmem((chunks, half, 2 * LANES), bf16),
            vmem((chunks, half, LANES), bf16),
            vmem((chunks, half, LANES), bf16),
            vmem((passing, width), bf16),
            vmem((passing, width), bf16),
            vmem((stripe, width), bf16),
            vmem((own, features), bf16),
            vmem((slots, features), bf16),
        ]
        + extra
        + [dma((layers * chunks,))] * 6
        + [dma((chunks,))] * 8
        + [dma((PARTS * line,))] * 2
        + [dma((PARTS * (bits + 1),))] * 4
        + [dma((PARTS * line,))] * 2
        + [dma((bits,))] * 2,
        compiler_params=pltpu.CompilerParams(
            collective_id=number, has_side_effects=True, vmem_limit_bytes=60 * 2**20
        ),
        cost_estimate=pl.CostEstimate(flops=flops, bytes_accessed=flops // 256, transcendentals=0),
    )(state, norm_gain, win, wout, *tables)


def mix(n_dp, n_mp, *args):
    (patch_query, key_cache, value_cache, cache_len, patch_end, ended_index, pool_out, norm_gain, w_in, w_out) = args
    layers, block_cols, _, hidden_local = w_in.shape
    win = w_in.transpose(0, 2, 1, 3)

    seq_rows = patch_query.shape[0]
    heads_width = key_cache.shape[2]
    place = lax.axis_index("mp")
    query_cols = lax.dynamic_slice_in_dim(patch_query, place * heads_width, heads_width, 1)
    attended = attend_local(query_cols, key_cache, value_cache, cache_len)
    picker = (ended_index[:, None] == jnp.arange(seq_rows, dtype=jnp.int32)[None, :]).astype(
        jnp.bfloat16
    )
    chosen = jnp.dot(picker, attended, preferred_element_type=jnp.float32).astype(jnp.bfloat16)
    partial_value = jnp.dot(chosen, pool_out, preferred_element_type=jnp.float32)
    pooled = own_rows_of_sum(partial_value.astype(jnp.bfloat16), n_mp)
    own = picker.shape[0] // n_mp
    reverse, bit = 0, 1
    while bit < n_mp:
        reverse = reverse * 2 + (place // bit) % 2
        bit *= 2
    own_picker = lax.dynamic_slice_in_dim(picker, reverse * own, own, 0)
    query_rows = jnp.dot(own_picker, patch_query, preferred_element_type=jnp.float32)

    slots = lax.all_gather(ended_index, "dp") < seq_rows
    filled = slots.reshape(n_dp // 2, 2, n_mp, own).transpose(2, 1, 0, 3).reshape(-1)
    count = filled.shape[0]
    index = jnp.arange(count, dtype=jnp.int32)
    before = (index[:, None] < index[None, :]).astype(jnp.bfloat16)
    ahead = jnp.dot(
        filled.astype(jnp.bfloat16)[None, :], before, preferred_element_type=jnp.float32
    )[0].astype(jnp.int32)
    place_of = jnp.where(filled, ahead, count)
    needed = jnp.sum(filled.astype(jnp.int32))
    sizes = [-(-count * k // 1024) * 32 for k in SIZES]
    which = sum((needed > size).astype(jnp.int32) for size in sizes[:-1])
    state = lax.switch(
        which,
        [functools.partial(run_layers, n_dp, n_mp, i, size) for i, size in enumerate(sizes)],
        query_rows + pooled, norm_gain, win, w_out, place_of,
    )
    placed = jnp.dot(picker.T, state, preferred_element_type=jnp.float32)
    return (placed * patch_end.astype(jnp.float32)[:, None]).astype(jnp.bfloat16)


def solution(mesh):
    in_specs = (
        P("dp", None),
        P("dp", None, "mp"),
        P("dp", None, "mp"),
        P("dp"),
        P("dp"),
        P("dp"),
        P("mp", None),
        P(),
        P(None, "dp", None, "mp"),
        P(None, "mp", "dp"),
    )
    out_specs = P("dp", None)
    def per_device(*args):
        return mix(mesh.shape["dp"], mesh.shape["mp"], *args)

    return jax.shard_map(
        per_device, mesh=mesh, in_specs=in_specs, out_specs=out_specs, check_vma=False
    )
```

```python
import functools

import jax
import jax.numpy as jnp
from jax import lax
from jax.experimental import pallas as pl
from jax.experimental.pallas import tpu as pltpu
from jax.sharding import PartitionSpec as P

HEAD_DIM = 128
LANES = 128
PARTS = 4
SIZES = (20, 23, 26, 32)
SKEW = 2
SKEW_HID = 2
EARLY = 5


norm_floor = 1e-05


def attend_local(query_cols, keys, values, lengths):
    seq_rows, patch_len, heads_width = keys.shape
    head_count = heads_width // HEAD_DIM
    query_heads = query_cols.reshape(seq_rows, head_count, HEAD_DIM)
    key_heads = keys.reshape(seq_rows, patch_len, head_count, HEAD_DIM)
    value_heads = values.reshape(seq_rows, patch_len, head_count, HEAD_DIM)
    scores = jnp.einsum(
        "shd,sphd->shp", query_heads, key_heads, preferred_element_type=jnp.float32
    ) * HEAD_DIM ** (-0.5)
    live_mask = jnp.arange(patch_len, dtype=jnp.int32)[None, None, :] < lengths[:, None, None]
    scores = jnp.where(live_mask, scores, jnp.float32(-1e30))
    top_score = jnp.max(scores, axis=2, keepdims=True)
    expo = jnp.where(live_mask, jnp.exp(scores - top_score), jnp.float32(0.0))
    weights = (expo / jnp.sum(expo, axis=2, keepdims=True)).astype(jnp.bfloat16)
    mixed = jnp.einsum("shp,sphd->shd", weights, value_heads, preferred_element_type=jnp.float32)
    return mixed.astype(jnp.bfloat16).reshape(seq_rows, heads_width)


def swap(value, axis, size, bit):
    return lax.ppermute(value, axis, [(i, i ^ bit) for i in range(size)])


def own_rows_of_sum(value, size):
    place = lax.axis_index("mp")
    bit = 1
    total = value.astype(jnp.float32)
    while bit < size:
        half = total.shape[0] // 2
        low = (place // bit) % 2
        kept = lax.dynamic_slice_in_dim(total, low * half, half, 0)
        given = lax.dynamic_slice_in_dim(total, (1 - low) * half, half, 0).astype(jnp.bfloat16)
        total = kept + swap(given, "mp", size, bit).astype(jnp.float32)
        bit *= 2
    return total


def layers_kernel(
    n_dp, n_mp, packed, *refs
):
    (state_in, gain_ref, win_ref, wout_ref, first_ref), refs = refs[:5], refs[5:]
    if packed:
        (pick, lay), refs = refs[:2], refs[2:]
    (out_ref, state, normed, feats, acc, w_up, w_down, right_buf, left_buf, right_hid, left_hid,
     give, got, share, back, final), refs = refs[:16], refs[16:]
    if packed:
        (live, total), refs = refs[:2], refs[2:]
    else:
        live, total = feats, acc
    (
    fl_sem, wl_sem, ws_sem, wr_sem, ol_sem, os_sem, or_sem,
    rs_sem, rr_sem, ls_sem, lr_sem, hrs_sem, hrr_sem, hls_sem, hlr_sem,
    az_s, az_r, ag_s, ag_r, dd_s, dd_r, dz_s, dz_r, ff_s, ff_r,
    ) = refs
    layers, chunks, _, full_width, _ = w_up.shape
    line = n_dp // 2
    bits = n_mp.bit_length() - 1
    block_cols = full_width // 2
    own = state.shape[0]
    stripe = line * own
    half_rows = right_buf.shape[1]
    dp, mp = lax.axis_index("dp"), lax.axis_index("mp")
    z, y = dp // 2, dp % 2
    top = line - 1
    reverse = 0
    for i in range(bits):
        reverse = reverse + ((mp // (1 << i)) % 2) * (1 << (bits - 1 - i))
    block = reverse * 2 + y

    def flip(value, bit):
        return value + bit - 2 * bit * ((value // bit) % 2)

    def partner(t):
        if t == 0:
            return (dp + 1 - 2 * y, mp)
        return (dp, flip(mp, 1 << (bits - t)))

    def at_line(other):
        return (other * 2 + y, mp)

    def send(src, dst, s_sem, r_sem, device):
        return pltpu.make_async_remote_copy(
            src_ref=src, dst_ref=dst, send_sem=s_sem, recv_sem=r_sem,
            device_id=device, device_id_type=pl.DeviceIdType.MESH,
        )

    barrier = pltpu.get_barrier_semaphore()
    for d in range(1, line):
        pl.semaphore_signal(
            barrier, inc=1, device_id=at_line((z + d) % line), device_id_type=pl.DeviceIdType.MESH
        )
    for t in range(bits + 1):
        pl.semaphore_signal(barrier, inc=1, device_id=partner(t), device_id_type=pl.DeviceIdType.MESH)
    pl.semaphore_wait(barrier, line - 1 + bits + 1)

    pieces = layers * chunks
    part_cols = full_width // PARTS

    def own_up(l, q):
        return pltpu.make_async_copy(
            win_ref.at[l, :, :, pl.ds(pl.multiple_of((y * chunks + q) * LANES, LANES), LANES)],
            w_up.at[l, q, :, pl.ds(y * block_cols, block_cols), :],
            wl_sem.at[l * chunks + q],
        )

    def own_down(l, q):
        return pltpu.make_async_copy(
            wout_ref.at[l, pl.ds((y * chunks + q) * LANES, LANES), :],
            w_down.at[l, q, y],
            ol_sem.at[l * chunks + q],
        )

    def give_up(l, q):
        return send(
            win_ref.at[l, :, :, pl.ds(pl.multiple_of(((1 - y) * chunks + q) * LANES, LANES), LANES)],
            w_up.at[l, q, :, pl.ds(y * block_cols, block_cols), :],
            ws_sem.at[l * chunks + q], wr_sem.at[l * chunks + q], partner(0),
        )

    def give_down(l, q):
        return send(
            wout_ref.at[l, pl.ds(((1 - y) * chunks + q) * LANES, LANES), :],
            w_down.at[l, q, y],
            os_sem.at[l * chunks + q], or_sem.at[l * chunks + q], partner(0),
        )

    early = first_ref.shape[2] // LANES

    def early_up(q):
        return pltpu.make_async_copy(
            first_ref.at[:, :, pl.ds(pl.multiple_of(q * LANES, LANES), LANES)],
            w_up.at[0, q, :, pl.ds((1 - y) * block_cols, block_cols), :],
            fl_sem.at[q],
        )

    def issue_up(piece):
        @pl.when(piece < pieces)
        def _():
            give_up(piece // chunks, piece % chunks).start()

    def start_own(piece, carry):
        own_up(piece // chunks, piece % chunks).start()
        own_down(piece // chunks, piece % chunks).start()
        return carry

    def start_early(q, carry):
        early_up(q).start()
        return carry

    lax.fori_loop(0, early, start_early, 0)
    lax.fori_loop(0, pieces, start_own, 0)

    state[...] = state_in[...]
    first_use = SKEW * jnp.minimum(z, top - z)
    first_down = SKEW_HID * jnp.minimum(z, top - z) + SKEW * top + 1
    steps = chunks + (SKEW + SKEW_HID) * top + 1
    def one_layer(l, carry):
        value = state[...]
        scale = lax.rsqrt(jnp.mean(value * value, axis=1, keepdims=True) + norm_floor)
        normed[...] = (value * scale * gain_ref[pl.ds(l, 1), :]).astype(jnp.bfloat16)
        mine = block * stripe + z * own
        next_up = early + l * (chunks + 5)

        def spread(c, d):
            other = (z + d) % line
            return send(
                normed.at[
                    :, pl.ds(pl.multiple_of(other * full_width + c * part_cols, LANES), part_cols)
                ],
                feats.at[
                    pl.ds(pl.multiple_of(mine, own), own), pl.ds(c * part_cols, part_cols)
                ],
                az_s.at[c * line + d], az_r.at[c * line + d], at_line(other),
            )

        def gather(c, t):
            rows = stripe << t
            start = pl.multiple_of((block // (1 << t)) * rows, stripe)
            ref = feats.at[
                pl.ds(start, rows), pl.ds(pl.multiple_of(c * part_cols, LANES), part_cols)
            ]
            at = c * (bits + 1) + t
            return send(ref, ref, ag_s.at[at], ag_r.at[at], partner(t))

        for c in range(PARTS):
            for d in range(1, line):
                spread(c, d).start()
        feats[pl.ds(pl.multiple_of(mine, own), own), :] = normed[
            :, pl.ds(pl.multiple_of(z * full_width, LANES), full_width)
        ]
        for t in range(bits + 1):
            for c in range(PARTS):
                if t == 0:
                    for d in range(1, line):
                        spread(c, d).wait_recv()
                else:
                    gather(c, t - 1).wait_recv()
                gather(c, t).start()
            if t == 0:
                for i in range(3):
                    issue_up(next_up + i)

        def arrived(c, inner):
            gather(c, bits).wait_recv()
            if packed:
                cols = pl.ds(pl.multiple_of(c * part_cols, LANES), part_cols)
                live[:, cols] = jnp.dot(
                    pick[...], feats[:, cols], preferred_element_type=jnp.float32
                ).astype(jnp.bfloat16)
            return inner

        lax.fori_loop(0, PARTS, arrived, 0)
        for c in range(PARTS):
            for d in range(1, line):
                spread(c, d).wait_send()
            for t in range(bits + 1):
                gather(c, t).wait_send()

        total[...] = jnp.zeros_like(total)

        def hidden_of(both):
            gate, up = both[:, :LANES], both[:, LANES:]
            return (gate / (1.0 + jnp.exp(-gate)) * up).astype(jnp.bfloat16)

        def chain(q, row0, first, last, to_next, to_prev, buf, hid, s_s, s_r, h_s, h_r):
            both = jnp.concatenate([w_up[l, q, 0], w_up[l, q, 1]], axis=1)
            part = jnp.dot(
                live[row0 : row0 + half_rows, :], both, preferred_element_type=jnp.float32
            )

            @pl.when(z == first)
            def _():
                buf[q] = part.astype(jnp.bfloat16)

            @pl.when(z != first)
            def _():
                send(buf.at[q], buf.at[q], s_s.at[q], s_r.at[q], at_line(to_next)).wait_recv()

            @pl.when(jnp.logical_and(z != first, z != last))
            def _():
                buf[q] = (part + buf[q].astype(jnp.float32)).astype(jnp.bfloat16)

            @pl.when(z == last)
            def _():
                hid[q] = hidden_of(part + buf[q].astype(jnp.float32))
                send(hid.at[q], hid.at[q], h_s.at[q], h_r.at[q], at_line(to_prev)).start()

            @pl.when(z != last)
            def _():
                send(buf.at[q], buf.at[q], s_s.at[q], s_r.at[q], at_line(to_next)).start()

        def pass_on(q, first, last, to_prev, hid, h_s, h_r):
            @pl.when(z != last)
            def _():
                send(hid.at[q], hid.at[q], h_s.at[q], h_r.at[q], at_line(to_prev)).wait_recv()

            @pl.when(jnp.logical_and(z != last, z != first))
            def _():
                send(hid.at[q], hid.at[q], h_s.at[q], h_r.at[q], at_line(to_prev)).start()

        def down(q, row0, hid):
            for c in range(2):
                cols = slice(c * block_cols, (c + 1) * block_cols)
                total[row0 : row0 + half_rows, cols] += jnp.dot(
                    hid[q], w_down[l, q, c], preferred_element_type=jnp.float32
                )

        nxt, prv = jnp.minimum(z + 1, top), jnp.maximum(z - 1, 0)

        def within(q):
            return jnp.logical_and(q >= 0, q < chunks)

        def one_step(s, inner):
            qw = s - first_use

            @pl.when(within(qw))
            def _():
                own_up(l, qw).wait()

                @pl.when(l * chunks + qw < early)
                def _():
                    early_up(qw).wait()

                @pl.when(l * chunks + qw >= early)
                def _():
                    give_up(l, qw).wait_recv()

            qd = s - first_down

            @pl.when(within(qd))
            def _():
                own_down(l, qd).wait()
                give_down(l, qd).wait_recv()

            qr = s - SKEW * z

            @pl.when(within(qr))
            def _():
                chain(qr, 0, 0, top, nxt, prv, right_buf, right_hid,
                      rs_sem, rr_sem, hrs_sem, hrr_sem)

            ql = s - SKEW * (top - z)

            @pl.when(within(ql))
            def _():
                chain(ql, half_rows, top, 0, prv, nxt, left_buf, left_hid,
                      ls_sem, lr_sem, hls_sem, hlr_sem)

            hr = s - (SKEW * top + 1) - SKEW_HID * (top - z)

            @pl.when(within(hr))
            def _():
                pass_on(hr, 0, top, prv, right_hid, hrs_sem, hrr_sem)

            hl = s - (SKEW * top + 1) - SKEW_HID * z

            @pl.when(within(hl))
            def _():
                pass_on(hl, top, 0, nxt, left_hid, hls_sem, hlr_sem)

            @pl.when(s < chunks)
            def _():
                issue_up(next_up + 3 + s)
                give_down(l, s).start()

            @pl.when(within(hr))
            def _():
                down(hr, 0, right_hid)

            @pl.when(within(hl))
            def _():
                down(hl, half_rows, left_hid)

            return inner

        lax.fori_loop(0, steps, one_step, 0)

        def drain(q, inner):
            @pl.when(z != top)
            def _():
                send(right_buf.at[q], right_buf.at[q], rs_sem.at[q], rr_sem.at[q],
                     at_line(nxt)).wait_send()

            @pl.when(z != 0)
            def _():
                send(left_buf.at[q], left_buf.at[q], ls_sem.at[q], lr_sem.at[q],
                     at_line(prv)).wait_send()

            @pl.when(z != 0)
            def _():
                send(right_hid.at[q], right_hid.at[q], hrs_sem.at[q], hrr_sem.at[q],
                     at_line(prv)).wait_send()

            @pl.when(z != top)
            def _():
                send(left_hid.at[q], left_hid.at[q], hls_sem.at[q], hlr_sem.at[q],
                     at_line(nxt)).wait_send()

            return inner

        lax.fori_loop(0, chunks, drain, 0)

        def side(t):
            return (block // (1 << t)) % 2

        def halve(c, t):
            rows = stripe << t
            at = stripe * ((1 << t) - 1)
            cols = pl.ds(pl.multiple_of(c * part_cols, LANES), part_cols)
            number = c * (bits + 1) + t
            return send(
                give.at[pl.ds(at, rows), cols], got.at[pl.ds(at, rows), cols],
                dd_s.at[number], dd_r.at[number], partner(t),
            )

        def start_halve(c, t):
            rows = stripe << t
            at = stripe * ((1 << t) - 1)
            cols = pl.ds(pl.multiple_of(c * part_cols, LANES), part_cols)
            there = pl.multiple_of((block // (1 << t) + 1 - 2 * side(t)) * rows, stripe)
            give[pl.ds(at, rows), cols] = acc[pl.ds(there, rows), cols].astype(jnp.bfloat16)
            halve(c, t).start()

        def bring(c, d):
            other = (z + d) % line
            return send(
                share.at[
                    pl.ds(pl.multiple_of(other * own, own), own), pl.ds(c * part_cols, part_cols)
                ],
                back.at[
                    :, pl.ds(pl.multiple_of(z * full_width + c * part_cols, LANES), part_cols)
                ],
                dz_s.at[c * line + d], dz_r.at[c * line + d], at_line(other),
            )

        def leave(c, inner):
            if packed:
                cols = pl.ds(pl.multiple_of(c * part_cols, LANES), part_cols)
                acc[:, cols] = jnp.dot(
                    lay[...], total[:, cols].astype(jnp.bfloat16), preferred_element_type=jnp.float32
                )
            start_halve(c, bits)
            return inner

        lax.fori_loop(0, PARTS, leave, 0)
        for t in range(bits, -1, -1):
            rows = stripe << t
            at = stripe * ((1 << t) - 1)
            here = pl.multiple_of((block // (1 << t)) * rows, stripe)
            for c in range(PARTS):
                cols = slice(c * part_cols, (c + 1) * part_cols)
                halve(c, t).wait_recv()
                acc[pl.ds(here, rows), cols] += got[at : at + rows, cols].astype(jnp.float32)
                if t > 0:
                    start_halve(c, t - 1)
                else:
                    share[:, cols] = acc[pl.ds(here, rows), cols].astype(jnp.bfloat16)
                    for d in range(1, line):
                        bring(c, d).start()
            if t == 1:
                issue_up(next_up + chunks + 3)
                issue_up(next_up + chunks + 4)
        columns = pl.ds(pl.multiple_of(z * full_width, LANES), full_width)
        back[:, columns] = share[pl.ds(pl.multiple_of(z * own, own), own), :]
        for c in range(PARTS):
            for d in range(1, line):
                bring(c, d).wait()
            for t in range(bits + 1):
                halve(c, t).wait_send()
        state[...] += back[...].astype(jnp.float32)
        return carry

    lax.fori_loop(0, layers, one_layer, 0)

    def drain_weights(piece, carry):
        @pl.when(piece >= early)
        def _():
            give_up(piece // chunks, piece % chunks).wait_send()

        give_down(piece // chunks, piece % chunks).wait_send()
        return carry

    lax.fori_loop(0, pieces, drain_weights, 0)

    final[pl.ds(pl.multiple_of(reverse * own, own), own), :] = state[...].astype(jnp.bfloat16)
    for t in range(bits):
        rows = own << t
        ref = final.at[pl.ds(pl.multiple_of((reverse // (1 << t)) * rows, own), rows), :]
        step = send(ref, ref, ff_s.at[t], ff_r.at[t], partner(t + 1))
        step.start()
        step.wait()
    out_ref[...] = final[...]


def run_layers(n_dp, n_mp, number, size, state, norm_gain, win, wout, first, place):
    layers, _, block_cols, hidden_local = win.shape
    own, features = state.shape
    chunks = hidden_local // 2 // LANES
    line = n_dp // 2
    bits = n_mp.bit_length() - 1
    width = 2 * block_cols
    rows = own * line * 2 * n_mp
    half = size // 2
    packed = size < rows
    slots = own * n_mp
    dma = pltpu.SemaphoreType.DMA
    vmem = pltpu.VMEM
    bf16, f32 = jnp.bfloat16, jnp.float32
    stripe = own * line
    passing = stripe * (2 * n_mp - 1)
    flops = 2 * layers * size * chunks * LANES * 3 * width
    tables, extra = [], []
    if packed:
        target = jnp.arange(size, dtype=jnp.int32)
        tables = [
            (target[:, None] == place[None, :]).astype(bf16),
            (place[:, None] == target[None, :]).astype(bf16),
        ]
        extra = [vmem((size, width), bf16), vmem((size, width), f32)]
    return pl.pallas_call(
        functools.partial(layers_kernel, n_dp, n_mp, packed),
        name="global_layers_%d" % number,
        out_shape=jax.ShapeDtypeStruct((slots, features), bf16),
        in_specs=[
            pl.BlockSpec(memory_space=pltpu.VMEM),
            pl.BlockSpec(memory_space=pltpu.VMEM),
            pl.BlockSpec(memory_space=pl.ANY),
            pl.BlockSpec(memory_space=pl.ANY),
            pl.BlockSpec(memory_space=pl.ANY),
        ]
        + [pl.BlockSpec(memory_space=pltpu.VMEM)] * len(tables),
        out_specs=pl.BlockSpec(memory_space=pltpu.VMEM),
        scratch_shapes=[
            vmem((own, features), f32),
            vmem((own, features), bf16),
            vmem((rows, width), bf16),
            vmem((rows, width), f32),
            vmem((layers, chunks, 2, width, LANES), bf16),
            vmem((layers, chunks, 2, LANES, block_cols), bf16),
            vmem((chunks, half, 2 * LANES), bf16),
            vmem((chunks, half, 2 * LANES), bf16),
            vmem((chunks, half, LANES), bf16),
            vmem((chunks, half, LANES), bf16),
            vmem((passing, width), bf16),
            vmem((passing, width), bf16),
            vmem((stripe, width), bf16),
            vmem((own, features), bf16),
            vmem((slots, features), bf16),
        ]
        + extra
        + [dma((first.shape[2] // LANES,))]
        + [dma((layers * chunks,))] * 6
        + [dma((chunks,))] * 8
        + [dma((PARTS * line,))] * 2
        + [dma((PARTS * (bits + 1),))] * 4
        + [dma((PARTS * line,))] * 2
        + [dma((bits,))] * 2,
        compiler_params=pltpu.CompilerParams(
            collective_id=number, has_side_effects=True, vmem_limit_bytes=60 * 2**20
        ),
        cost_estimate=pl.CostEstimate(flops=flops, bytes_accessed=flops // 256, transcendentals=0),
    )(state, norm_gain, win, wout, first, *tables)


def mix(n_dp, n_mp, *args):
    (patch_query, key_cache, value_cache, cache_len, patch_end, ended_index, pool_out, norm_gain, w_in, w_out) = args
    layers, block_cols, _, hidden_local = w_in.shape
    win = w_in.transpose(0, 2, 1, 3)
    half = hidden_local // 2
    early = min(EARLY, half // LANES - 1) * LANES
    start = (1 - lax.axis_index("dp") % 2) * half
    given = lax.dynamic_slice(win, (0, 0, 0, start), (1, 2, block_cols, early))
    first = swap(given, "dp", n_dp, 1)[0]

    seq_rows = patch_query.shape[0]
    heads_width = key_cache.shape[2]
    place = lax.axis_index("mp")
    query_cols = lax.dynamic_slice_in_dim(patch_query, place * heads_width, heads_width, 1)
    attended = attend_local(query_cols, key_cache, value_cache, cache_len)
    picker = (ended_index[:, None] == jnp.arange(seq_rows, dtype=jnp.int32)[None, :]).astype(
        jnp.bfloat16
    )
    chosen = jnp.dot(picker, attended, preferred_element_type=jnp.float32).astype(jnp.bfloat16)
    partial_value = jnp.dot(chosen, pool_out, preferred_element_type=jnp.float32)
    pooled = own_rows_of_sum(partial_value.astype(jnp.bfloat16), n_mp)
    own = picker.shape[0] // n_mp
    reverse, bit = 0, 1
    while bit < n_mp:
        reverse = reverse * 2 + (place // bit) % 2
        bit *= 2
    own_picker = lax.dynamic_slice_in_dim(picker, reverse * own, own, 0)
    query_rows = jnp.dot(own_picker, patch_query, preferred_element_type=jnp.float32)

    table = ended_index[None, :]
    at, bit = lax.axis_index("dp"), 1
    while bit < n_dp:
        other = swap(table, "dp", n_dp, bit)
        low = (at // bit) % 2 == 0
        table = jnp.concatenate(
            [jnp.where(low, table, other), jnp.where(low, other, table)], axis=0
        )
        bit *= 2
    slots = table < seq_rows
    filled = slots.reshape(n_dp // 2, 2, n_mp, own).transpose(2, 1, 0, 3).reshape(-1)
    count = filled.shape[0]
    index = jnp.arange(count, dtype=jnp.int32)
    before = (index[:, None] < index[None, :]).astype(jnp.bfloat16)
    ahead = jnp.dot(
        filled.astype(jnp.bfloat16)[None, :], before, preferred_element_type=jnp.float32
    )[0].astype(jnp.int32)
    place_of = jnp.where(filled, ahead, count)
    needed = jnp.sum(filled.astype(jnp.int32))
    sizes = [-(-count * k // 1024) * 32 for k in SIZES]
    which = sum((needed > size).astype(jnp.int32) for size in sizes[:-1])
    state = lax.switch(
        which,
        [functools.partial(run_layers, n_dp, n_mp, i, size) for i, size in enumerate(sizes)],
        query_rows + pooled, norm_gain, win, w_out, first, place_of,
    )
    placed = jnp.dot(picker.T, state, preferred_element_type=jnp.float32)
    return (placed * patch_end.astype(jnp.float32)[:, None]).astype(jnp.bfloat16)


def solution(mesh):
    in_specs = (
        P("dp", None),
        P("dp", None, "mp"),
        P("dp", None, "mp"),
        P("dp"),
        P("dp"),
        P("dp"),
        P("mp", None),
        P(),
        P(None, "dp", None, "mp"),
        P(None, "mp", "dp"),
    )
    out_specs = P("dp", None)
    def per_device(*args):
        return mix(mesh.shape["dp"], mesh.shape["mp"], *args)

    return jax.shard_map(
        per_device, mesh=mesh, in_specs=in_specs, out_specs=out_specs, check_vma=False
    )
```
